512 devices in a mesh: dp: 64 (over z_hi, x, y), expert: 8 (over z_lo, core).
Axes of the slice: x: 4, y: 8, z: 8 (z_hi: 2, z_lo: 4; z = z_hi * 4 + z_lo), core: 2. Of those that a mesh axis runs over, the one named last changes fastest.
Arguments:
- tokens: bfloat16 [65536, 3072], P('dp'), may hold values from -16 to 16
- hidden_grads: bfloat16 [65536, 1024], P('dp', 'expert'), may hold values from -6 to 6
- routed: int32 [64], P('dp'), may hold values from 1 to 1024, 49152 in all
- master: float32 [2, 8192, 3072], P(None, 'expert', 'dp'), may hold values from -6 to 6
- moment_one: float32 [2, 1024, 3072], P(None, 'expert', 'dp'), may hold values from -3 to 3
- moment_two: float32 [2, 1024, 3072], P(None, 'expert', 'dp'), may hold values from 0.05 to 1
- hot_units: int32 [1024], P('expert'), may hold values from 0 to 1023, as said below
- cold_blocks: float32 [2, 8192, 3072], P(None, 'expert', 'dp'), may hold values from -6 to 6
- cold_shift: int32 [8192], P('expert'), may hold values from 0 to 7, as said below
Outputs:
- new_master: float32 [2, 8192, 3072], P(None, 'expert', 'dp')
- new_moment_one: float32 [2, 1024, 3072], P(None, 'expert', 'dp')
- new_moment_two: float32 [2, 1024, 3072], P(None, 'expert', 'dp')
The draws below stay inside these ranges and needn't reach their ends.
Inputs may be any that keep to these rules, and one draw needn't show every extreme that they name: `routed`: the counts sum to 49152 and one of them equals 1024. `hot_units`: within each aligned block of 128 entries the values are distinct. `cold_shift`: within each aligned block of 1024 entries every value occurs exactly 8192 // 8 // 8 times.
All inputs are finite; a program needn't handle non-finite values. No bound on the sum of `routed` on one device may be relied on, other than what follows from the above.
Results may differ from the reference program's by a relative error of at most 0.003.
Values may be sent and summed in bfloat16 or wider, within the bound.
A program may use at most 64 MiB of HBM per device.

```python
import math
import jax
import jax.numpy as jnp
import numpy as np

D = 3072
UNITS = 8192
HOT_DEV = 128
TOK_DEV = 1024
RANKS = 64
CYCLE = 8
TOKENS = 65536
HOT = 1024


def draw_hot_units(key, part):
    blocks = HOT // HOT_DEV
    span = UNITS // blocks
    keys = jax.random.split(jax.random.fold_in(key, 17), blocks)

    def pick_block(block_key):
        return jax.random.permutation(block_key, span)[:HOT_DEV]
    picks = jax.vmap(pick_block)(keys)
    return picks.reshape(HOT).astype(jnp.int32)


def draw_cold_shift(key, part):
    span = UNITS // CYCLE
    keys = jax.random.split(jax.random.fold_in(key, 29), CYCLE)

    def shift_block(block_key):
        return jax.random.permutation(block_key, span) % CYCLE
    shifts = jax.vmap(shift_block)(keys)
    return shifts.reshape(UNITS).astype(jnp.int32)


def strengthened(array, own_key, source, target, parts, factor):
    owner, partner = [(jnp.arange(array.shape[axis_at]) // (array.shape[axis_at] // parts)).reshape([-1 if axis == axis_at else 1 for axis in range(array.ndim)]) for axis_at in (source, target)]
    chosen = jax.random.permutation(own_key, parts)[partner]
    strong = (owner == chosen) | (owner == (partner + parts // 2) % parts)
    return jnp.where(strong, factor * array, array)


def level_of(key, extent, cuts, low, high):
    def one(dim, shards_of):
        heights = jax.random.uniform(jax.random.fold_in(jax.random.fold_in(key, 6), dim), (shards_of,), jnp.float32, low / len(cuts), high / len(cuts))
        return jnp.repeat(jnp.exp(heights), extent[dim] // shards_of).reshape((-1,) + (1,) * (len(extent) - dim - 1))

    gain = one(*cuts[0])
    for cut in cuts[1:]:
        gain = gain * one(*cut)
    return gain


def split_up(number_of, total, limit, skew):
    weights = [(1 << 20) // math.isqrt(grade ** skew) + 1 for grade in range(2, number_of + 1)]
    spare, given = total - limit - (number_of - 1), [1] * (number_of - 1)
    while spare > 0:
        free = [i for i in range(number_of - 1) if given[i] < limit]
        mass, left = sum([weights[i] for i in free]), spare
        for i in free:
            addition = min(limit - given[i], max(1, left * weights[i] // mass), spare)
            given[i] = given[i] + addition
            spare = spare - addition
    return np.array([limit] + given)


def ragged(own_key, number_of, total, bound, slope):
    if number_of == 2:
        one = jax.random.randint(own_key, (), max(1, total - bound), min(bound, total - 1) + 1)
        return jnp.stack([one, total - one])
    sizes = jnp.asarray(split_up(number_of, total, bound, slope), jnp.int32)
    twos = (number_of - 1) // 2
    donor, sink = sizes[1:1 + 2 * twos:2], sizes[2:2 + 2 * twos:2]
    room = jnp.minimum(donor - 1, bound - sink)
    shifted = jax.random.randint(jax.random.fold_in(own_key, 1), (twos,), 0, 1 << 20) % (room + 1)
    sizes = sizes.at[1:1 + 2 * twos:2].set(donor - shifted).at[2:2 + 2 * twos:2].set(sink + shifted)
    return sizes[jax.random.permutation(jax.random.fold_in(own_key, 2), number_of)]


def gaussian(own_key, shape, spread, limit, cuts=(), kind=jnp.bfloat16):
    loudness = level_of(own_key, shape, cuts, -0.22, 0.18) if cuts else 1.0
    entries = jax.random.normal(own_key, shape, jnp.float32) * spread * loudness
    return jnp.minimum(jnp.maximum(entries, -limit), limit).astype(kind)


def bell_draw_with(stream_key, dims, width, bound, pieces, heavy, kind=jnp.bfloat16):
    entries = width * jax.random.normal(stream_key, dims, jnp.float32)
    if pieces:
        entries = entries * level_of(stream_key, dims, pieces, -0.22, 0.18)
    return jnp.clip(strengthened(entries, jax.random.fold_in(stream_key, 3), *heavy), -bound, bound).astype(kind)


def setup_inputs(seed: int = 0) -> dict:
    seeds = jax.random.split(jax.random.key(seed), 10)
    tokens = bell_draw_with(seeds[0], (TOKENS, D), 1.0, 16.0, ((0, 64),), (0, 1, 64, 4.0))
    hidden_grads = gaussian(seeds[1], (TOKENS, HOT), 1.0, 6.0, ((0, 64), (1, 8)))
    routed = ragged(seeds[2], RANKS, 3 * TOK_DEV * RANKS // 4, TOK_DEV, 2).astype(jnp.int32)
    master = gaussian(seeds[3], (2, UNITS, D), 1.0, 6.0, ((1, 8), (2, 64)), jnp.float32)
    moment_one = gaussian(seeds[4], (2, HOT, D), 0.3, 3.0, ((1, 8), (2, 64)), jnp.float32)
    moment_two = jnp.clip(jnp.exp(math.log(1.0) - 2.9957323 * jax.random.uniform(seeds[5], (2, HOT, D), jnp.float32) ** level_of(seeds[5], (2, HOT, D), ((1, 8), (2, 64)), -0.2, 0.2)), 0.05, 1.0)
    hot_units = draw_hot_units(jax.random.fold_in(seeds[9], 71), 0)
    cold_blocks = gaussian(seeds[7], (2, UNITS, D), 1.0, 6.0, ((1, 8), (2, 64)), jnp.float32)
    cold_shift = draw_cold_shift(jax.random.fold_in(seeds[9], 71), 0)
    return dict(tokens=tokens, hidden_grads=hidden_grads, routed=routed, master=master, moment_one=moment_one, moment_two=moment_two, hot_units=hot_units, cold_blocks=cold_blocks, cold_shift=cold_shift)


beta_one = 0.9
beta_two = 0.95
step_rate = 0.1
adam_eps = 1e-08

def reference(tokens, hidden_grads, routed, master, moment_one, moment_two, hot_units, cold_blocks, cold_shift):
    span = UNITS // CYCLE
    weight_scale = D ** (-0.5)
    block_of = jnp.arange(HOT, dtype=jnp.int32) // HOT_DEV
    hot_global = (block_of * span + hot_units).astype(jnp.int32)
    master_hot = master[:, hot_global, :]
    weights = master_hot.astype(jnp.bfloat16)
    slots = jnp.arange(TOK_DEV, dtype=jnp.int32)
    live_rows = (slots[None, :] < routed[:, None]).astype(jnp.float32).reshape(TOKENS, 1)
    gate_pre = jnp.dot(tokens, weights[0].T, preferred_element_type=jnp.float32) * weight_scale
    up_pre = jnp.dot(tokens, weights[1].T, preferred_element_type=jnp.float32) * weight_scale
    cotangent = hidden_grads.astype(jnp.float32)
    sigmoid = jax.nn.sigmoid(gate_pre)
    d_up = (live_rows * cotangent * gate_pre * sigmoid).astype(jnp.bfloat16)
    d_gate = (live_rows * cotangent * up_pre * sigmoid * (1.0 + gate_pre * (1.0 - sigmoid))).astype(jnp.bfloat16)
    grads = jnp.stack([jnp.dot(d_gate.T, tokens, preferred_element_type=jnp.float32), jnp.dot(d_up.T, tokens, preferred_element_type=jnp.float32)]) * weight_scale
    first_new = beta_one * moment_one + (1.0 - beta_one) * grads
    second_new = beta_two * moment_two + (1.0 - beta_two) * grads * grads
    adam = master_hot - step_rate * first_new / (jnp.sqrt(second_new) + adam_eps)
    unit_index = jnp.arange(UNITS, dtype=jnp.int32)
    source = (unit_index // span - cold_shift) % CYCLE
    src_index = (source * span + unit_index % span).astype(jnp.int32)
    received = cold_blocks[:, src_index, :]
    new_master = received.at[:, hot_global, :].set(adam)
    return (new_master, first_new, second_new)
```

```python
import functools

import jax
import jax.numpy as jnp
from jax import lax
from jax.experimental import pallas as pl
from jax.experimental.pallas import tpu as pltpu
from jax.sharding import Mesh
from jax.sharding import PartitionSpec as P

D = 3072
DP = ("dp_0", "dp_1", "dp_2")
MESH = pl.DeviceIdType.MESH

beta_one = 0.9
beta_two = 0.95
step_rate = 0.1
adam_eps = 1e-08

SPLIT = 16

Z_TIME = 5.5
AX_TIME, AY_HOP = 2.7, 2.6
BY_TIME, BX_HOP = 5.2, 3.8
COLD_TIME = 9.05
TURN_TIME, TURN_STEP = 3.0, 1.1
RAY_HOP, RAX_TIME = 2.8, 3.0
RBX_HOP, RBY_HOP = 4.2, 2.6
COLD_BACK = 8.0

F32 = jnp.float32
BF16 = jnp.bfloat16


def nn(a, b):
    return lax.dot_general(a, b, (((1,), (0,)), ((), ())), preferred_element_type=F32)


def nt(a, b):
    return lax.dot_general(a, b, (((1,), (1,)), ((), ())), preferred_element_type=F32)


def thirds(v):
    high = v.astype(BF16)
    rest = v - high.astype(F32)
    mid = rest.astype(BF16)
    low = (rest - mid.astype(F32)).astype(BF16)
    return jnp.concatenate([high, mid, low], axis=0)


def joined(v):
    rows = v.shape[0] // 3
    return v[:rows] + (v[rows : 2 * rows] + v[2 * rows :])


def one_hot(cond):
    return jnp.where(cond, 1.0, 0.0).astype(BF16)


def iota(shape, dim):
    return lax.broadcasted_iota(jnp.int32, shape, dim)


def kernel(
    dims,
    tok_hbm,
    hidden,
    routed,
    master,
    hot,
    cold,
    shift,
    grads_out,
    received_out,
    hot_out,
    tok,
    tok_t,
    wt,
    acc,
    dmat,
    part,
    hot_pick,
    unpack,
    cold_three,
    shifts,
    count_buf,
    cold_sent,
    cold_got,
    received,
    b_send,
    b_recv,
    a_send,
    a_recv,
    a_sum,
    b_sum,
    by_send,
    by_recv,
    ax_recv,
    plane_sum,
    z_recv,
    tok_sem,
    out_sem,
    ag_send_sem,
    ag_recv_sem,
    rs_send_sem,
    rs_recv_sem,
    cold_send_sem,
    cold_recv_sem,
):
    Z, X, Y, E, W, H, SPAN = dims
    YW = Y * W
    z, x, y = (lax.axis_index(a) for a in DP)
    e = lax.axis_index("expert")
    s = 1 - 2 * lax.rem(e, 2)

    def xi(k):
        return lax.rem(x + k * s + 2 * X, X)

    def yi(k):
        return lax.rem(y + k * s + 2 * Y, Y)

    def at_x(k):
        return (z, xi(k), y, e)

    def at_y(k):
        return (z, x, yi(k), e)

    def at_e(k):
        return (z, x, y, lax.rem(e + k, E))

    z_peer = (1 - z, x, y, e)
    peers = [at_x(k) for k in range(1, X)] + [at_y(k) for k in range(1, Y)]
    peers += [z_peer] + [at_e(k) for k in range(1, E)]

    barrier = pltpu.get_barrier_semaphore()
    for peer in peers:
        pl.semaphore_signal(barrier, inc=1, device_id=peer, device_id_type=MESH)
    tok_copy = pltpu.make_async_copy(tok_hbm, tok, tok_sem)
    tok_copy.start()

    hot_pick[...] = one_hot(iota((SPAN, H), 0) == hot[...])
    whole = master[...].reshape(2 * W, SPAN)
    picked = nn(whole.astype(BF16), hot_pick[...]).astype(BF16)
    wt[z, x, y, :, 0:H] = picked[:W]
    wt[z, x, y, :, H : 2 * H] = picked[W:]
    shifts[e] = shift[...]

    pl.semaphore_wait(barrier, len(peers))

    pending = []

    def send(src, dst, sems, k, peer):
        copy = pltpu.make_async_remote_copy(
            src_ref=src,
            dst_ref=dst,
            send_sem=sems[0].at[k],
            recv_sem=sems[1].at[k],
            device_id=peer,
            device_id_type=MESH,
        )
        copy.start()
        pending.append(copy)

    def arrived(dst, sems, k):
        pltpu.make_async_remote_copy(
            src_ref=dst,
            dst_ref=dst,
            send_sem=sems[0].at[k],
            recv_sem=sems[1].at[k],
            device_id=z_peer,
            device_id_type=MESH,
        ).wait_recv()

    events = []

    def at(t, fn):
        events.append((t, len(events), fn))

    def run():
        for _, _, fn in sorted(events, key=lambda ev: ev[:2]):
            fn()
        events.clear()

    px, mx, py, my = X // 2, X // 2 - 1, Y // 2, Y // 2 - 1

    def slots(p):
        off = [1 + p * 2 * (X + Y - 2)]
        for n in (py, my, X - 1, px, mx, Y - 1):
            off.append(off[-1] + n)
        return off

    low, high = pl.ds(0, SPLIT), pl.ds(SPLIT, W - SPLIT)

    ag = (ag_send_sem, ag_recv_sem)

    def zp(p):
        return z if p == 0 else 1 - z

    def gather_plane(p, t0):
        pz = zp(p)
        ay_plus, ay_minus, ax, bx_plus, bx_minus, by, _ = slots(p)

        def piece_a(kx):
            return wt.at[pz, xi(kx), y, low]

        def piece_b(ky):
            return wt.at[pz, x, yi(ky), high]

        def row_a(ky):
            return wt.at[pz, :, yi(ky), low]

        def row_b(kx):
            return wt.at[pz, xi(kx), :, high]

        def first():
            for k in range(1, X):
                send(piece_a(0), piece_a(0), ag, ax + k - 1, at_x(k))
            for k in range(1, Y):
                send(piece_b(0), piece_b(0), ag, by + k - 1, at_y(k))

        at(t0, first)

        def all_a():
            for k in range(1, X):
                arrived(piece_a(-k), ag, ax + k - 1)

        def all_b():
            for k in range(1, Y):
                arrived(piece_b(-k), ag, by + k - 1)

        def ring(block, peer_of, plus, minus, o_plus, o_minus, t, hop):
            def begin():
                if plus:
                    send(block(0), block(0), ag, o_plus, peer_of(1))
                if minus:
                    send(block(0), block(0), ag, o_minus, peer_of(-1))

            at(t, begin)
            for d in range(1, max(plus, minus) + 1):

                def step(d=d):
                    if d <= plus:
                        arrived(block(-d), ag, o_plus + d - 1)
                        if d < plus:
                            send(block(-d), block(-d), ag, o_plus + d, peer_of(1))
                    if d <= minus:
                        arrived(block(d), ag, o_minus + d - 1)
                        if d < minus:
                            send(block(d), block(d), ag, o_minus + d, peer_of(-1))

                at(t + d * hop, step)
            return t + max(plus, minus) * hop

        ta = t0 + AX_TIME
        at(ta, all_a)
        ta = ring(row_a, at_y, py, my, ay_plus, ay_minus, ta + 0.001, AY_HOP)
        tb = t0 + BY_TIME
        at(tb, all_b)
        tb = ring(row_b, at_x, px, mx, bx_plus, bx_minus, tb + 0.001, BX_HOP)
        return max(ta, tb)

    own = wt.at[z, x, y]
    at(0.0, lambda: send(own, own, ag, 0, z_peer))
    t_own = gather_plane(0, 0.001)
    at(Z_TIME, lambda: arrived(wt.at[1 - z, x, y], ag, 0))
    t_far = gather_plane(1, Z_TIME + 0.001)

    cs = (cold_send_sem, cold_recv_sem)

    def shift_out():
        for k in range(1, E):
            send(shift, shifts.at[e], cs, k, at_e(k))

    at(0.1, shift_out)

    def before():
        return one_hot(iota((SPAN, SPAN), 0) < iota((SPAN, SPAN), 1))

    def prepare_unpack():
        mine = shift[...]
        rows = iota((E, SPAN), 0)
        mask = mine == rows
        count = nn(one_hot(mask), before())
        rank = jnp.sum(jnp.where(mask, count, 0.0), axis=0, keepdims=True).astype(jnp.int32)
        slot = lax.rem(e - mine + E, E) * (SPAN // E) + rank
        unpack[...] = one_hot(iota((SPAN, SPAN), 0) == slot)

    at(0.2, prepare_unpack)

    def hot_exact():
        hot_out[...] = joined(nn(thirds(master[...].reshape(2 * W, SPAN)), hot_pick[...]))

    at(0.3, hot_exact)

    def cold_count():
        cold_three[...] = thirds(cold[...].reshape(2 * W, SPAN))
        for k in range(1, E):
            arrived(shifts.at[lax.rem(e - k + E, E)], cs, k)
        rows = iota((E, SPAN), 0)
        mask = shifts[...].reshape(E, SPAN) == lax.rem(rows - e + E, E)
        count = nn(one_hot(mask), before()).astype(jnp.int32)
        count_buf[...] = jnp.where(mask, count, -1)

    at(COLD_TIME, cold_count)

    def cold_pack(b):
        pick = one_hot(iota((SPAN // E, SPAN), 0) == count_buf[b : b + 1])
        cold_sent[b] = joined(nt(cold_three[...], pick))

    for b in range(E):
        at(COLD_TIME + 0.2 + 0.3 * b, functools.partial(cold_pack, b))

    def cold_out():
        for k in range(1, E):
            b = lax.rem(e + k, E)
            send(cold_sent.at[b], cold_got.at[e], cs, E + k, at_e(k))
        cold_got[e] = cold_sent[e]

    at(COLD_TIME + 0.2 + 0.3 * E, cold_out)

    def turn_tokens(c):
        cols = pl.ds(c * YW, YW)
        tok_t[cols, :] = tok[:, cols].T

    at(0.4, tok_copy.wait)
    for c in range(Z * X):
        at(TURN_TIME + TURN_STEP * c, functools.partial(turn_tokens, c))

    def forward(p, first):
        def body(c, _):
            cols = pl.ds(pl.multiple_of((zp(p) * X + c) * YW, 128), YW)
            term = nn(tok[:, cols], wt[zp(p), c].reshape(YW, 2 * H))
            if first:
                acc[...] = term
            else:
                acc[...] += term
            return 0

        if first:
            body(0, 0)
            first = False
            lax.fori_loop(1, X, body, 0)
        else:
            lax.fori_loop(0, X, body, 0)

    at(t_own + 0.1, lambda: forward(0, True))
    at(t_far + 0.1, lambda: forward(1, False))
    run()

    scale = D ** (-0.5)
    TOK = tok.shape[0]
    STEP = 128

    def cotangent(i, _):
        rows = pl.ds(pl.multiple_of(i * STEP, STEP), STEP)
        gate = acc[rows, 0:H] * scale
        up = acc[rows, H : 2 * H] * scale
        c = hidden[rows, :].astype(F32)
        live = (iota((STEP, H), 0) + i * STEP) < routed[...]
        c = jnp.where(live, c, 0.0)
        sig = jax.nn.sigmoid(gate)
        dmat[rows, H : 2 * H] = (c * gate * sig).astype(BF16)
        dmat[rows, 0:H] = (c * up * sig * (1.0 + gate * (1.0 - sig))).astype(BF16)
        return 0

    lax.fori_loop(0, TOK // STEP, cotangent, 0)

    rs = (rs_send_sem, rs_recv_sem)

    def backward(p, kx):
        rows = pl.ds(pl.multiple_of((zp(p) * X + xi(kx)) * YW, 128), YW)
        part[p, xi(kx)] = nn(tok_t[rows, :], dmat[...]).reshape(Y, W, 2 * H)

    def reduce_ring(p, term, peer_of, plus, minus, o_plus, o_minus, sbuf, rbuf, t, hop, done):
        def one(k, count, base, o, sign):
            value = term(sign * (count - k))
            if k:
                arrived(rbuf.at[p, base + k - 1], rs, o + k - 1)
                value = value + rbuf[p, base + k - 1].astype(F32)
            sbuf[p, base + k] = value.astype(sbuf.dtype)
            send(sbuf.at[p, base + k], rbuf.at[p, base + k], rs, o + k, peer_of(sign))

        for k in range(max(plus, minus)):

            def step(k=k):
                if k < plus:
                    one(k, plus, 0, o_plus, 1)
                if k < minus:
                    one(k, minus, plus, o_minus, -1)

            at(t + k * hop, step)

        def last():
            value = term(0)
            for count, base, o in ((plus, 0, o_plus), (minus, plus, o_minus)):
                if count:
                    arrived(rbuf.at[p, base + count - 1], rs, o + count - 1)
                    value = value + rbuf[p, base + count - 1].astype(F32)
            done(value)

        t = t + max(plus, minus) * hop
        at(t, last)
        return t

    def reduce_plane(p, t_a, t_b):
        ay_plus, ay_minus, ax, bx_plus, bx_minus, by, _ = slots(p)

        def set_a(v):
            a_sum[p] = v
            for k in range(1, X):
                send(a_sum.at[p, xi(k)], ax_recv.at[p, k - 1], rs, ax + k - 1, at_x(k))

        def set_b(v):
            b_sum[p] = v

        def end_a():
            value = a_sum[p, x]
            for k in range(1, X):
                arrived(ax_recv.at[p, k - 1], rs, ax + k - 1)
                value = value + ax_recv[p, k - 1]
            plane_sum[p, 0:SPLIT] = value

        def end_b(v):
            plane_sum[p, SPLIT:W] = v

        ta = reduce_ring(
            p, lambda k: part[p, :, yi(k), 0:SPLIT, :],
            at_y, py, my, ay_plus, ay_minus, a_send, a_recv, t_a, RAY_HOP, set_a,
        ) + RAX_TIME
        at(ta, end_a)
        tb = reduce_ring(
            p, lambda k: part[p, xi(k), :, SPLIT:W, :],
            at_x, px, mx, bx_plus, bx_minus, b_send, b_recv, t_b, RBX_HOP, set_b,
        )
        tb = reduce_ring(
            p, lambda k: b_sum[p, yi(k)],
            at_y, py, my, by, by + py, by_send, by_recv, tb + 0.001, RBY_HOP, end_b,
        )
        return max(ta, tb)

    for i in range(px + mx):
        k = px - i if i < px else -1 - (i - px)
        k = (px, *range(-mx, 0), *range(px - 1, 0, -1))[i]
        at(-2.0 + 0.1 * i, functools.partial(backward, 1, k))
        at(0.5 + 0.1 * i, functools.partial(backward, 0, k))
    at(-1.5, functools.partial(backward, 1, 0))
    at(1.0, functools.partial(backward, 0, 0))
    t_far = reduce_plane(1, -1.4, -1.85)
    at(t_far + 0.01, lambda: send(plane_sum.at[1], z_recv, rs, 0, z_peer))
    reduce_plane(0, 1.1, 0.65)

    out_copy = pltpu.make_async_copy(received, received_out, out_sem)

    def cold_in():
        for k in range(1, E):
            arrived(cold_got.at[lax.rem(e - k + E, E)], cs, E + k)
        got = jnp.concatenate([cold_got[c] for c in range(E)], axis=1)
        received[...] = joined(nn(thirds(got), unpack[...]))
        out_copy.start()

    at(COLD_BACK, cold_in)
    run()

    arrived(z_recv, rs, 0)
    grads_out[...] = (plane_sum[0] + z_recv[...]) * scale
    out_copy.wait()
    for copy in pending:
        copy.wait_send()


def update(grads, m1, m2, hot, master_hot, received, out, m1_out, m2_out):
    _, W, H = m1.shape
    SPAN = received.shape[1]
    pick = one_hot(iota((SPAN, H), 0) == hot[...])
    for i in range(2):
        g = grads[:, i * H : (i + 1) * H]
        first = beta_one * m1[i] + (1.0 - beta_one) * g
        second = beta_two * m2[i] + (1.0 - beta_two) * g * g
        adam = master_hot[i * W : (i + 1) * W] - step_rate * first / (jnp.sqrt(second) + adam_eps)
        m1_out[i] = first
        m2_out[i] = second
        spread = joined(nt(thirds(adam), pick))
        is_hot = nt(jnp.ones((8, H), BF16), pick)[0:1] > 0.5
        out[i] = jnp.where(is_hot, spread, received[i * W : (i + 1) * W])


def per_device(
    tokens, hidden_grads, routed, master, moment_one, moment_two, hot_units, cold_blocks, cold_shift
):
    Z, X, Y = (lax.axis_size(a) for a in DP)
    E = lax.axis_size("expert")
    W = master.shape[2]
    H = hot_units.shape[0]
    SPAN = master.shape[1]
    TOK = tokens.shape[0]
    dims = (Z, X, Y, E, W, H, SPAN)
    vmem = pl.BlockSpec(memory_space=pltpu.VMEM)
    copies = 1 + 2 * 2 * (X + Y - 2)
    dma = pltpu.SemaphoreType.DMA
    V = pltpu.VMEM
    HI = W - SPLIT
    scratch = [
        V((TOK, D), BF16),
        V((D, TOK), BF16),
        V((Z, X, Y, W, 2 * H), BF16),
        V((TOK, 2 * H), F32),
        V((TOK, 2 * H), BF16),
        V((2, X, Y, W, 2 * H), F32),
        V((SPAN, H), BF16),
        V((SPAN, SPAN), BF16),
        V((6 * W, SPAN), BF16),
        V((E, 1, SPAN), jnp.int32),
        V((E, SPAN), jnp.int32),
        V((E, 2 * W, SPAN // E), F32),
        V((E, 2 * W, SPAN // E), F32),
        V((2 * W, SPAN), F32),
        V((2, X - 1, Y, HI, 2 * H), BF16),
        V((2, X - 1, Y, HI, 2 * H), BF16),
        V((2, Y - 1, X, SPLIT, 2 * H), BF16),
        V((2, Y - 1, X, SPLIT, 2 * H), BF16),
        V((2, X, SPLIT, 2 * H), F32),
        V((2, Y, HI, 2 * H), F32),
        V((2, Y - 1, HI, 2 * H), F32),
        V((2, Y - 1, HI, 2 * H), F32),
        V((2, X - 1, SPLIT, 2 * H), F32),
        V((2, W, 2 * H), F32),
        V((W, 2 * H), F32),
        dma,
        dma,
        dma((copies,)),
        dma((copies,)),
        dma((copies,)),
        dma((copies,)),
        dma((2 * E,)),
        dma((2 * E,)),
    ]

    def turned(v):
        return v.transpose(0, 2, 1)

    hot_row = hot_units.reshape(1, H)
    hbm = pl.BlockSpec(memory_space=pl.ANY)
    grads, received, master_hot = pl.pallas_call(
        functools.partial(kernel, dims),
        out_shape=(
            jax.ShapeDtypeStruct((W, 2 * H), F32),
            jax.ShapeDtypeStruct((2 * W, SPAN), F32),
            jax.ShapeDtypeStruct((2 * W, H), F32),
        ),
        in_specs=[hbm] + [vmem] * 6,
        out_specs=(vmem, hbm, vmem),
        scratch_shapes=scratch,
        compiler_params=pltpu.CompilerParams(
            collective_id=0, has_side_effects=True, vmem_limit_bytes=60 * 1024 * 1024
        ),
        name="expert_step",
    )(
        tokens,
        hidden_grads,
        routed.reshape(1, 1),
        turned(master),
        hot_row,
        turned(cold_blocks),
        cold_shift.reshape(1, SPAN),
    )
    outs = pl.pallas_call(
        update,
        out_shape=(
            jax.ShapeDtypeStruct((2, W, SPAN), F32),
            jax.ShapeDtypeStruct((2, W, H), F32),
            jax.ShapeDtypeStruct((2, W, H), F32),
        ),
        in_specs=[vmem] * 6,
        out_specs=(vmem, vmem, vmem),
        name="update",
    )(grads, turned(moment_one), turned(moment_two), hot_row, master_hot, received)
    return tuple(turned(v) for v in outs)


def solution(mesh):
    finer = Mesh(
        mesh.devices.reshape(2, 4, 8, mesh.shape["expert"]), ("dp_0", "dp_1", "dp_2", "expert")
    )
    placed = (
        P(DP, None),
        P(DP, "expert"),
        P(DP),
        P(None, "expert", DP),
        P(None, "expert", DP),
        P(None, "expert", DP),
        P("expert"),
        P(None, "expert", DP),
        P("expert"),
    )
    return jax.shard_map(
        per_device,
        mesh=finer,
        in_specs=placed,
        out_specs=(P(None, "expert", DP), P(None, "expert", DP), P(None, "expert", DP)),
        check_vma=False,
    )
```

```python
import functools

import jax
import jax.numpy as jnp
from jax import lax
from jax.experimental import pallas as pl
from jax.experimental.pallas import tpu as pltpu
from jax.sharding import Mesh
from jax.sharding import PartitionSpec as P

D = 3072
DP = ("dp_0", "dp_1", "dp_2")
MESH = pl.DeviceIdType.MESH

beta_one = 0.9
beta_two = 0.95
step_rate = 0.1
adam_eps = 1e-08

SPLIT = 16

STEP_ONE, STEP_TWO = 3.2, 4.2
COLD_TIME = 8.0
TURN_TIME, TURN_STEP = 1.0, 1.3
COLD_BACK = 9.5

F32 = jnp.float32
BF16 = jnp.bfloat16


def nn(a, b):
    return lax.dot_general(a, b, (((1,), (0,)), ((), ())), preferred_element_type=F32)


def nt(a, b):
    return lax.dot_general(a, b, (((1,), (1,)), ((), ())), preferred_element_type=F32)


def thirds(v):
    high = v.astype(BF16)
    rest = v - high.astype(F32)
    mid = rest.astype(BF16)
    low = (rest - mid.astype(F32)).astype(BF16)
    return jnp.concatenate([high, mid, low], axis=0)


def joined(v):
    rows = v.shape[0] // 3
    return v[:rows] + (v[rows : 2 * rows] + v[2 * rows :])


def one_hot(cond):
    return jnp.where(cond, 1.0, 0.0).astype(BF16)


def iota(shape, dim):
    return lax.broadcasted_iota(jnp.int32, shape, dim)


def kernel(
    dims,
    tok_hbm,
    hidden_hbm,
    routed_hbm,
    master_hbm,
    hot_hbm,
    cold_hbm,
    shift_hbm,
    grads_out,
    received_out,
    hot_out,
    tok,
    hidden,
    routed,
    master,
    hot,
    cold,
    shift,
    tok_t,
    wt,
    acc,
    dmat,
    part,
    hot_pick,
    unpack,
    cold_three,
    shifts,
    count_buf,
    cold_sent,
    cold_got,
    received,
    b_send,
    b_recv,
    a_send,
    a_recv,
    a_sum,
    b_sum,
    bz_send,
    bz_recv,
    by_recv,
    ax_recv,
    az_recv,
    in_sem,
    out_sem,
    ag_send_sem,
    ag_recv_sem,
    rs_send_sem,
    rs_recv_sem,
    cold_send_sem,
    cold_recv_sem,
):
    Z, X, Y, E, W, H, SPAN = dims
    YW = Y * W
    z, x, y = (lax.axis_index(a) for a in DP)
    e = lax.axis_index("expert")
    s = 1 - 2 * lax.rem(e, 2)
    xs = [lax.rem(x + k * s + 2 * X, X) for k in range(X)]
    ys = [lax.rem(y + k * s + 2 * Y, Y) for k in range(Y)]
    es = [lax.rem(e + k, E) for k in range(E)]

    def xi(k):
        return xs[k % X]

    def yi(k):
        return ys[k % Y]

    def at_x(k, p=0):
        return (z if p == 0 else 1 - z, xi(k), y, e)

    def at_y(k, p=0):
        return (z if p == 0 else 1 - z, x, yi(k), e)

    def at_e(k):
        return (z, x, y, es[k])

    far_last = sorted(range(Y), key=lambda k: (min(k, Y - k), k))
    peers = [at_y(k, 1) for k in reversed(far_last)] + [at_x(k, 1) for k in range(1, X)]
    peers += [at_y(k) for k in range(1, Y)] + [at_x(k) for k in range(1, X)]
    peers += [at_e(k) for k in range(1, E)]

    barrier = pltpu.get_barrier_semaphore()
    for peer in peers:
        pl.semaphore_signal(barrier, inc=1, device_id=peer, device_id_type=MESH)
    ins = []
    for i, (src, dst) in enumerate(
        (
            (hot_hbm, hot),
            (master_hbm, master),
            (shift_hbm, shift),
            (tok_hbm, tok),
            (cold_hbm, cold),
            (hidden_hbm, hidden),
            (routed_hbm, routed),
        )
    ):
        ins.append(pltpu.make_async_copy(src, dst, in_sem.at[i]))
    for copy in ins[:3]:
        copy.start()

    for copy in ins[:3]:
        copy.wait()
    for copy in ins[3:]:
        copy.start()
    hot_pick[...] = one_hot(iota((SPAN, H), 0) == hot[...])
    whole = master[...].reshape(2 * W, SPAN)
    picked = nn(whole.astype(BF16), hot_pick[...]).astype(BF16)
    wt[z, x, y, :, 0:H] = picked[:W]
    wt[z, x, y, :, H : 2 * H] = picked[W:]
    shifts[e] = shift[...]

    pl.semaphore_wait(barrier, len(peers))

    pending = []

    class Family:
        def __init__(self, send_sem, recv_sem):
            self.sems = (send_sem, recv_sem)
            self.names = {}

        def copy(self, src, dst, name, peer):
            k = self.names.setdefault(name, len(self.names))
            assert k < self.sems[0].shape[0]
            return pltpu.make_async_remote_copy(
                src_ref=src,
                dst_ref=dst,
                send_sem=self.sems[0].at[k],
                recv_sem=self.sems[1].at[k],
                device_id=peer,
                device_id_type=MESH,
            )

        def send(self, src, dst, name, peer):
            copy = self.copy(src, dst, name, peer)
            copy.start()
            pending.append(copy)

        def arrived(self, dst, name):
            self.copy(dst, dst, name, at_x(0, 1)).wait_recv()

    events = []

    def at(t, fn):
        events.append((t, len(events), fn))

    def run():
        for _, _, fn in sorted(events, key=lambda ev: ev[:2]):
            fn()
        events.clear()

    low, high = pl.ds(0, SPLIT), pl.ds(SPLIT, W - SPLIT)

    ag = Family(ag_send_sem, ag_recv_sem)

    def zp(p):
        return z if p == 0 else 1 - z

    def first_sends():
        mine_a, mine_b = wt.at[z, x, y, low], wt.at[z, x, y, high]
        for k in range(X):
            ag.send(mine_a, mine_a, ("ax", 1, k), at_x(k, 1))
        for k in range(1, X):
            ag.send(mine_a, mine_a, ("ax", 0, k), at_x(k))
        for k in far_last[1:]:
            ag.send(mine_b, mine_b, ("by", 0, k), at_y(k))
        for k in far_last:
            ag.send(mine_b, mine_b, ("by", 1, k), at_y(k, 1))

    at(0.0, first_sends)

    def gather_a(p, t):
        def row(k):
            return wt.at[zp(p), :, yi(k), low]

        def begin():
            for k in range(p ^ 1, X):
                ag.arrived(wt.at[zp(p), xi(-k), y, low], ("ax", p, k))
            for k in (2, 1, -2, -1):
                ag.send(row(0), row(0), ("ay", p, k), at_y(k))

        def near():
            for k in (1, -1):
                ag.arrived(row(-k), ("ay", p, k))

        def relay():
            ag.arrived(row(-2), ("ay", p, 2))
            ag.send(row(-2), row(-2), ("ay", p, 4), at_y(2))
            ag.send(row(-2), row(-2), ("ay", p, 3), at_y(1))
            ag.arrived(row(2), ("ay", p, -2))
            ag.send(row(2), row(2), ("ay", p, -3), at_y(-1))

        def end():
            for k in (3, -3, 4):
                ag.arrived(row(-k), ("ay", p, k))

        at(t, begin)
        at(t + STEP_TWO + 0.4, relay)
        at(t + STEP_TWO + 0.6, near)
        at(t + 2 * STEP_TWO + 1.5, end)
        return t + 2 * STEP_TWO + 1.5

    def gather_b(p, t, ky):
        def piece(kx):
            return wt.at[zp(p), xi(kx), yi(-ky), high]

        def begin():
            if ky or p:
                ag.arrived(piece(0), ("by", p, ky))
            ag.send(piece(0), piece(0), ("bx", p, ky, 1), at_x(1))
            ag.send(piece(0), piece(0), ("bx", p, ky, -1), at_x(-1))

        def relay():
            ag.arrived(piece(-1), ("bx", p, ky, 1))
            ag.send(piece(-1), piece(-1), ("bx", p, ky, 2), at_x(1))

        def end():
            ag.arrived(piece(1), ("bx", p, ky, -1))
            ag.arrived(piece(-2), ("bx", p, ky, 2))

        at(t, begin)
        at(t + STEP_ONE + 0.3, relay)
        at(t + 2 * STEP_ONE + 0.8, end)
        return t + 2 * STEP_ONE + 0.8

    ends = [[gather_a(0, 4.3)], [gather_a(1, 8.3)]]
    for i, k in enumerate(far_last):
        d = min(k, Y - k)
        ends[0].append(gather_b(0, 0.01 if k == 0 else 2.4 + 0.8 * d + 0.3 * i, k))
        ends[1].append(gather_b(1, 6.6 + 0.8 * d + 0.4 * i, k))
    t_own, t_far = max(ends[0]), max(ends[1])

    cs = Family(cold_send_sem, cold_recv_sem)

    def shift_out():
        for k in range(1, E):
            cs.send(shift, shifts.at[e], ("s", k), at_e(k))

    at(0.02, shift_out)

    def before():
        return one_hot(iota((SPAN, SPAN), 0) < iota((SPAN, SPAN), 1))

    def prepare_unpack():
        mine = shift[...]
        rows = iota((E, SPAN), 0)
        mask = mine == rows
        count = nn(one_hot(mask), before())
        rank = jnp.sum(jnp.where(mask, count, 0.0), axis=0, keepdims=True).astype(jnp.int32)
        slot = lax.rem(e - mine + E, E) * (SPAN // E) + rank
        unpack[...] = one_hot(iota((SPAN, SPAN), 0) == slot)

    at(0.2, prepare_unpack)

    def hot_exact():
        hot_out[...] = joined(nn(thirds(master[...].reshape(2 * W, SPAN)), hot_pick[...]))

    at(0.3, hot_exact)

    def cold_split():
        ins[4].wait()
        cold_three[...] = thirds(cold[...].reshape(2 * W, SPAN))

    at(0.6, cold_split)

    def cold_count():
        for k in range(1, E):
            cs.arrived(shifts.at[es[E - k]], ("s", k))
        rows = iota((E, SPAN), 0)
        mask = shifts[...].reshape(E, SPAN) == lax.rem(rows - e + E, E)
        count = nn(one_hot(mask), before()).astype(jnp.int32)
        count_buf[...] = jnp.where(mask, count, -1)

    at(COLD_TIME, cold_count)

    def cold_pack(b):
        pick = one_hot(iota((SPAN // E, SPAN), 0) == count_buf[b : b + 1])
        cold_sent[b] = joined(nt(cold_three[...], pick))

    for b in range(E):
        at(COLD_TIME + 0.4 + 0.5 * b, functools.partial(cold_pack, b))

    def cold_out():
        for k in range(1, E):
            cs.send(cold_sent.at[es[k]], cold_got.at[e], ("c", k), at_e(k))
        cold_got[e] = cold_sent[e]

    at(COLD_TIME + 0.4 + 0.5 * E, cold_out)

    def turn_tokens(c):
        cols = pl.ds(c * YW, YW)
        tok_t[cols, :] = tok[:, cols].T

    at(0.4, lambda: ins[3].wait())
    for c in range(Z * X):
        at(TURN_TIME + TURN_STEP * c, functools.partial(turn_tokens, c))

    def forward(p):
        def body(c, _):
            cols = pl.ds(pl.multiple_of((zp(p) * X + c) * YW, 128), YW)
            acc[...] += nn(tok[:, cols], wt[zp(p), c].reshape(YW, 2 * H))
            return 0

        lax.fori_loop(0, X, body, 0)

    def clear():
        acc[...] = jnp.zeros_like(acc)

    at(0.5, clear)
    at(t_own + 0.1, lambda: forward(0))
    at(t_far + 0.1, lambda: forward(1))
    run()

    scale = D ** (-0.5)
    TOK = tok.shape[0]
    STEP = 128
    ins[5].wait()
    ins[6].wait()
    count = routed[0]

    def cotangent(i, _):
        rows = pl.ds(pl.multiple_of(i * STEP, STEP), STEP)
        gate = acc[rows, 0:H] * scale
        up = acc[rows, H : 2 * H] * scale
        c = hidden[rows, :].astype(F32)
        live = (iota((STEP, H), 0) + i * STEP) < count
        c = jnp.where(live, c, 0.0)
        sig = jax.nn.sigmoid(gate)
        dmat[rows, H : 2 * H] = (c * gate * sig).astype(BF16)
        dmat[rows, 0:H] = (c * up * sig * (1.0 + gate * (1.0 - sig))).astype(BF16)
        return 0

    lax.fori_loop(0, TOK // STEP, cotangent, 0)

    rs = Family(rs_send_sem, rs_recv_sem)

    def backward(p, kx):
        rows = pl.ds(pl.multiple_of((zp(p) * X + xi(kx)) * YW, 128), YW)
        part[p, xi(kx)] = nn(tok_t[rows, :], dmat[...]).reshape(Y, W, 2 * H)

    def reduce_a(p, t):
        def term(k):
            return part[p, :, yi(k), 0:SPLIT, :]

        def go(i, value, k):
            a_send[p, i] = value.astype(BF16)
            rs.send(a_send.at[p, i], a_recv.at[p, i], ("ay", p, i), at_y(k))

        def come(i):
            rs.arrived(a_recv.at[p, i], ("ay", p, i))
            return a_recv[p, i].astype(F32)

        def begin():
            go(4, term(4), 2)
            go(3, term(3), 1)
            go(6, term(-3), -1)
            go(0, term(1), 1)
            go(5, term(-1), -1)

        def middle():
            go(1, term(2) + come(3) + come(4), 2)
            go(2, term(-2) + come(6), -2)

        def end():
            a_sum[p] = term(0) + come(0) + come(5) + come(1) + come(2)
            for k in range(X):
                if p:
                    rs.send(a_sum.at[p, xi(k)], az_recv.at[k], ("ax", p, k), at_x(k, 1))
                elif k:
                    rs.send(a_sum.at[p, xi(k)], ax_recv.at[k - 1], ("ax", p, k), at_x(k))

        at(t, begin)
        at(t + STEP_TWO + 0.8, middle)
        at(t + 2 * STEP_TWO + 1.5, end)

    HALF = Y // 2

    def reduce_b(p, t):
        def half(h, t):
            cut = pl.ds(h * HALF, HALF)

            def term(k):
                return part[p, xi(k), cut, SPLIT:W, :]

            def go(i, value, k):
                b_send[p, i, cut] = value.astype(BF16)
                rs.send(b_send.at[p, i, cut], b_recv.at[p, i, cut], ("bx", p, i, h), at_x(k))

            def come(i):
                rs.arrived(b_recv.at[p, i, cut], ("bx", p, i, h))
                return b_recv[p, i, cut].astype(F32)

            def begin():
                go(0, term(2), 1)
                go(2, term(-1), -1)

            def middle():
                go(1, term(1) + come(0), 1)

            def end():
                b_sum[p, cut] = term(0) + come(1) + come(2)

            at(t, begin)
            at(t + STEP_ONE + 1.4, middle)
            at(t + 2 * STEP_ONE + 3.0, end)

        half(0, t)
        half(1, t + 0.3)

        def spread():
            if p:
                bz_send[...] = b_sum[p].astype(BF16)
            for k in reversed(far_last):
                if p:
                    rs.send(bz_send.at[yi(k)], bz_recv.at[k], ("by", p, k), at_y(k, 1))
                elif k:
                    rs.send(b_sum.at[p, yi(k)], by_recv.at[k - 1], ("by", p, k), at_y(k))

        at(t + 2 * STEP_ONE + 3.31, spread)

    for i, k in enumerate((2, -1, 1, 0)):
        at(-2.0 + 0.1 * i, functools.partial(backward, 1, k))
        at(0.5 + 0.1 * i, functools.partial(backward, 0, k))
    reduce_b(1, -1.85)
    reduce_a(1, -1.4)
    reduce_b(0, 0.65)
    reduce_a(0, 1.1)

    out_copy = pltpu.make_async_copy(received, received_out, out_sem)

    def cold_in():
        for k in range(1, E):
            cs.arrived(cold_got.at[es[E - k]], ("c", k))
        got = jnp.concatenate([cold_got[c] for c in range(E)], axis=1)
        received[...] = joined(nn(thirds(got), unpack[...]))
        out_copy.start()

    at(COLD_BACK, cold_in)
    run()

    value = a_sum[0, x]
    for k in range(1, X):
        rs.arrived(ax_recv.at[k - 1], ("ax", 0, k))
        value = value + ax_recv[k - 1]
    for k in range(X):
        rs.arrived(az_recv.at[k], ("ax", 1, k))
        value = value + az_recv[k]
    grads_out[0:SPLIT] = value * scale
    value = b_sum[0, y]
    for k in range(1, Y):
        rs.arrived(by_recv.at[k - 1], ("by", 0, k))
        value = value + by_recv[k - 1]
    for k in range(Y):
        rs.arrived(bz_recv.at[k], ("by", 1, k))
        value = value + bz_recv[k].astype(F32)
    grads_out[SPLIT:W] = value * scale
    out_copy.wait()
    for copy in pending:
        copy.wait_send()


def update(grads, m1, m2, hot, master_hot, received, out, m1_out, m2_out):
    _, W, H = m1.shape
    SPAN = received.shape[1]
    pick = one_hot(iota((SPAN, H), 0) == hot[...])
    for i in range(2):
        g = grads[:, i * H : (i + 1) * H]
        first = beta_one * m1[i] + (1.0 - beta_one) * g
        second = beta_two * m2[i] + (1.0 - beta_two) * g * g
        adam = master_hot[i * W : (i + 1) * W] - step_rate * first / (jnp.sqrt(second) + adam_eps)
        m1_out[i] = first
        m2_out[i] = second
        spread = joined(nt(thirds(adam), pick))
        is_hot = nt(jnp.ones((8, H), BF16), pick)[0:1] > 0.5
        out[i] = jnp.where(is_hot, spread, received[i * W : (i + 1) * W])


def per_device(
    tokens, hidden_grads, routed, master, moment_one, moment_two, hot_units, cold_blocks, cold_shift
):
    Z, X, Y = (lax.axis_size(a) for a in DP)
    E = lax.axis_size("expert")
    W = master.shape[2]
    H = hot_units.shape[0]
    SPAN = master.shape[1]
    TOK = tokens.shape[0]
    dims = (Z, X, Y, E, W, H, SPAN)
    vmem = pl.BlockSpec(memory_space=pltpu.VMEM)
    dma = pltpu.SemaphoreType.DMA
    V = pltpu.VMEM
    HI = W - SPLIT
    ag_copies = 2 * ((X + Y) + (Y - 1) + Y * (X - 1))
    rs_copies = 2 * ((Y - 1) + 2 * (X - 1) + X + Y)
    scratch = [
        V((TOK, D), BF16),
        V((TOK, H), BF16),
        pltpu.SMEM((1,), jnp.int32),
        V((2, W, SPAN), F32),
        V((1, H), jnp.int32),
        V((2, W, SPAN), F32),
        V((1, SPAN), jnp.int32),
        V((D, TOK), BF16),
        V((Z, X, Y, W, 2 * H), BF16),
        V((TOK, 2 * H), F32),
        V((TOK, 2 * H), BF16),
        V((2, X, Y, W, 2 * H), F32),
        V((SPAN, H), BF16),
        V((SPAN, SPAN), BF16),
        V((6 * W, SPAN), BF16),
        V((E, 1, SPAN), jnp.int32),
        V((E, SPAN), jnp.int32),
        V((E, 2 * W, SPAN // E), F32),
        V((E, 2 * W, SPAN // E), F32),
        V((2 * W, SPAN), F32),
        V((2, X - 1, Y, HI, 2 * H), BF16),
        V((2, X - 1, Y, HI, 2 * H), BF16),
        V((2, Y - 1, X, SPLIT, 2 * H), BF16),
        V((2, Y - 1, X, SPLIT, 2 * H), BF16),
        V((2, X, SPLIT, 2 * H), F32),
        V((2, Y, HI, 2 * H), F32),
        V((Y, HI, 2 * H), BF16),
        V((Y, HI, 2 * H), BF16),
        V((Y - 1, HI, 2 * H), F32),
        V((X - 1, SPLIT, 2 * H), F32),
        V((X, SPLIT, 2 * H), F32),
        dma((7,)),
        dma,
        dma((ag_copies,)),
        dma((ag_copies,)),
        dma((rs_copies,)),
        dma((rs_copies,)),
        dma((2 * E,)),
        dma((2 * E,)),
    ]

    def turned(v):
        return v.transpose(0, 2, 1)

    hot_row = hot_units.reshape(1, H)
    grads, received, master_hot = pl.pallas_call(
        functools.partial(kernel, dims),
        out_shape=(
            jax.ShapeDtypeStruct((W, 2 * H), F32),
            jax.ShapeDtypeStruct((2 * W, SPAN), F32),
            jax.ShapeDtypeStruct((2 * W, H), F32),
        ),
        in_specs=[pl.BlockSpec(memory_space=pltpu.HBM)] * 7,
        out_specs=(vmem, pl.BlockSpec(memory_space=pltpu.HBM), vmem),
        scratch_shapes=scratch,
        compiler_params=pltpu.CompilerParams(
            collective_id=0, has_side_effects=True, vmem_limit_bytes=60 * 1024 * 1024
        ),
        name="expert_step",
    )(
        tokens,
        hidden_grads,
        routed,
        turned(master),
        hot_row,
        turned(cold_blocks),
        cold_shift.reshape(1, SPAN),
    )
    outs = pl.pallas_call(
        update,
        out_shape=(
            jax.ShapeDtypeStruct((2, W, SPAN), F32),
            jax.ShapeDtypeStruct((2, W, H), F32),
            jax.ShapeDtypeStruct((2, W, H), F32),
        ),
        in_specs=[vmem] * 6,
        out_specs=(vmem, vmem, vmem),
        name="update",
    )(grads, turned(moment_one), turned(moment_two), hot_row, master_hot, received)
    return tuple(turned(v) for v in outs)


def solution(mesh):
    finer = Mesh(
        mesh.devices.reshape(2, 4, 8, mesh.shape["expert"]), ("dp_0", "dp_1", "dp_2", "expert")
    )
    placed = (
        P(DP, None),
        P(DP, "expert"),
        P(DP),
        P(None, "expert", DP),
        P(None, "expert", DP),
        P(None, "expert", DP),
        P("expert"),
        P(None, "expert", DP),
        P("expert"),
    )
    return jax.shard_map(
        per_device,
        mesh=finer,
        in_specs=placed,
        out_specs=(P(None, "expert", DP), P(None, "expert", DP), P(None, "expert", DP)),
        check_vma=False,
    )
```

```python
import functools

import jax
import jax.numpy as jnp
from jax import lax
from jax.experimental import pallas as pl
from jax.experimental.pallas import tpu as pltpu
from jax.sharding import Mesh
from jax.sharding import PartitionSpec as P

D = 3072
DP = ("dp_0", "dp_1", "dp_2")
MESH = pl.DeviceIdType.MESH

beta_one = 0.9
beta_two = 0.95
step_rate = 0.1
adam_eps = 1e-08

SPLIT = 16

STEP_ONE, STEP_TWO = 3.2, 4.2
COLD_TIME = 8.0
TURN_TIME, TURN_STEP = 1.0, 1.3
COLD_BACK = 9.5

F32 = jnp.float32
BF16 = jnp.bfloat16


def nn(a, b):
    return lax.dot_general(a, b, (((1,), (0,)), ((), ())), preferred_element_type=F32)


def nt(a, b):
    return lax.dot_general(a, b, (((1,), (1,)), ((), ())), preferred_element_type=F32)


def thirds(v):
    high = v.astype(BF16)
    rest = v - high.astype(F32)
    mid = rest.astype(BF16)
    low = (rest - mid.astype(F32)).astype(BF16)
    return jnp.concatenate([high, mid, low], axis=0)


def joined(v):
    rows = v.shape[0] // 3
    return v[:rows] + (v[rows : 2 * rows] + v[2 * rows :])


def one_hot(cond):
    return jnp.where(cond, 1.0, 0.0).astype(BF16)


def iota(shape, dim):
    return lax.broadcasted_iota(jnp.int32, shape, dim)


def kernel(
    dims,
    tok_hbm,
    hidden_hbm,
    routed_hbm,
    master_hbm,
    hot_hbm,
    cold_hbm,
    shift_hbm,
    grads_out,
    received_out,
    hot_out,
    tok,
    hidden,
    routed,
    master,
    hot,
    cold,
    shift,
    tok_t,
    wt,
    acc,
    dmat,
    part,
    hot_pick,
    unpack,
    cold_three,
    shifts,
    count_buf,
    cold_sent,
    cold_got,
    received,
    b_send,
    b_recv,
    a_send,
    a_recv,
    a_sum,
    b_sum,
    bz_send,
    bz_recv,
    by_recv,
    ax_recv,
    az_recv,
    in_sem,
    out_sem,
    ag_send_sem,
    ag_recv_sem,
    rs_send_sem,
    rs_recv_sem,
    cold_send_sem,
    cold_recv_sem,
):
    Z, X, Y, E, W, H, SPAN = dims
    YW = Y * W
    z, x, y = (lax.axis_index(a) for a in DP)
    e = lax.axis_index("expert")
    s = 1 - 2 * lax.rem(e, 2)
    xs = [lax.rem(x + k * s + 2 * X, X) for k in range(X)]
    ys = [lax.rem(y + k * s + 2 * Y, Y) for k in range(Y)]
    es = [lax.rem(e + k, E) for k in range(E)]

    def xi(k):
        return xs[k % X]

    def yi(k):
        return ys[k % Y]

    def at_x(k, p=0):
        return (z if p == 0 else 1 - z, xi(k), y, e)

    def at_y(k, p=0):
        return (z if p == 0 else 1 - z, x, yi(k), e)

    def at_e(k):
        return (z, x, y, es[k])

    far_last = sorted(range(Y), key=lambda k: (min(k, Y - k), k))
    peers = [at_x(0, 1)] + [at_y(k) for k in reversed(far_last[1:])]
    peers += [at_x(k) for k in range(1, X)] + [at_e(k) for k in range(1, E)]

    barrier = pltpu.get_barrier_semaphore()
    for peer in peers:
        pl.semaphore_signal(barrier, inc=1, device_id=peer, device_id_type=MESH)
    ins = []
    for i, (src, dst) in enumerate(
        (
            (hot_hbm, hot),
            (master_hbm, master),
            (shift_hbm, shift),
            (tok_hbm, tok),
            (cold_hbm, cold),
            (hidden_hbm, hidden),
            (routed_hbm, routed),
        )
    ):
        ins.append(pltpu.make_async_copy(src, dst, in_sem.at[i]))
    for copy in ins[:3]:
        copy.start()

    for copy in ins[:3]:
        copy.wait()
    for copy in ins[3:]:
        copy.start()
    hot_pick[...] = one_hot(iota((SPAN, H), 0) == hot[...])
    whole = master[...].reshape(2 * W, SPAN)
    picked = nn(whole.astype(BF16), hot_pick[...]).astype(BF16)
    wt[z, x, y, :, 0:H] = picked[:W]
    wt[z, x, y, :, H : 2 * H] = picked[W:]
    shifts[e] = shift[...]

    pl.semaphore_wait(barrier, len(peers))

    pending = []

    class Family:
        def __init__(self, send_sem, recv_sem):
            self.sems = (send_sem, recv_sem)
            self.names = {}

        def copy(self, src, dst, name, peer):
            k = self.names.setdefault(name, len(self.names))
            assert k < self.sems[0].shape[0]
            return pltpu.make_async_remote_copy(
                src_ref=src,
                dst_ref=dst,
                send_sem=self.sems[0].at[k],
                recv_sem=self.sems[1].at[k],
                device_id=peer,
                device_id_type=MESH,
            )

        def send(self, src, dst, name, peer):
            copy = self.copy(src, dst, name, peer)
            copy.start()
            pending.append(copy)

        def arrived(self, dst, name):
            self.copy(dst, dst, name, at_x(0, 1)).wait_recv()

    events = []

    def at(t, fn):
        events.append((t, len(events), fn))

    def run():
        for _, _, fn in sorted(events, key=lambda ev: ev[:2]):
            fn()
        events.clear()

    low, high = pl.ds(0, SPLIT), pl.ds(SPLIT, W - SPLIT)

    ag = Family(ag_send_sem, ag_recv_sem)

    def zp(p):
        return z if p == 0 else 1 - z

    def first_sends(p):
        mine = wt.at[zp(p), x, y]
        if p:
            ag.arrived(mine, ("z",))
        else:
            ag.send(mine, mine, ("z",), at_x(0, 1))
        mine_a, mine_b = wt.at[zp(p), x, y, low], wt.at[zp(p), x, y, high]
        for k in range(1, X):
            ag.send(mine_a, mine_a, ("ax", p, k), at_x(k))
        for k in far_last[1:]:
            ag.send(mine_b, mine_b, ("by", p, k), at_y(k))

    Z_TIME = 5.8
    at(0.0, lambda: first_sends(0))
    at(Z_TIME, lambda: first_sends(1))

    def gather_a(p, t):
        def row(k):
            return wt.at[zp(p), :, yi(k), low]

        def begin():
            for k in range(1, X):
                ag.arrived(wt.at[zp(p), xi(-k), y, low], ("ax", p, k))
            for k in (2, 1, -2, -1):
                ag.send(row(0), row(0), ("ay", p, k), at_y(k))

        def near():
            for k in (1, -1):
                ag.arrived(row(-k), ("ay", p, k))

        def relay():
            ag.arrived(row(-2), ("ay", p, 2))
            ag.send(row(-2), row(-2), ("ay", p, 4), at_y(2))
            ag.send(row(-2), row(-2), ("ay", p, 3), at_y(1))
            ag.arrived(row(2), ("ay", p, -2))
            ag.send(row(2), row(2), ("ay", p, -3), at_y(-1))

        def end():
            for k in (3, -3, 4):
                ag.arrived(row(-k), ("ay", p, k))

        at(t, begin)
        at(t + STEP_TWO + 0.4, relay)
        at(t + STEP_TWO + 0.6, near)
        at(t + 2 * STEP_TWO + 1.5, end)
        return t + 2 * STEP_TWO + 1.5

    def gather_b(p, t, ky):
        def piece(kx):
            return wt.at[zp(p), xi(kx), yi(-ky), high]

        def begin():
            if ky:
                ag.arrived(piece(0), ("by", p, ky))
            ag.send(piece(0), piece(0), ("bx", p, ky, 1), at_x(1))
            ag.send(piece(0), piece(0), ("bx", p, ky, -1), at_x(-1))

        def relay():
            ag.arrived(piece(-1), ("bx", p, ky, 1))
            ag.send(piece(-1), piece(-1), ("bx", p, ky, 2), at_x(1))

        def end():
            ag.arrived(piece(1), ("bx", p, ky, -1))
            ag.arrived(piece(-2), ("bx", p, ky, 2))

        at(t, begin)
        at(t + STEP_ONE + 0.3, relay)
        at(t + 2 * STEP_ONE + 0.8, end)
        return t + 2 * STEP_ONE + 0.8

    ends = [[gather_a(0, 4.3)], [gather_a(1, Z_TIME + 4.3)]]
    for i, k in enumerate(far_last):
        d = min(k, Y - k)
        for p in range(2):
            t = 0.01 if k == 0 else 2.4 + 0.8 * d + 0.3 * i
            ends[p].append(gather_b(p, t + p * Z_TIME, k))
    t_own, t_far = max(ends[0]), max(ends[1])

    cs = Family(cold_send_sem, cold_recv_sem)

    def shift_out():
        for k in range(1, E):
            cs.send(shift, shifts.at[e], ("s", k), at_e(k))

    at(0.02, shift_out)

    def before():
        return one_hot(iota((SPAN, SPAN), 0) < iota((SPAN, SPAN), 1))

    def prepare_unpack():
        mine = shift[...]
        rows = iota((E, SPAN), 0)
        mask = mine == rows
        count = nn(one_hot(mask), before())
        rank = jnp.sum(jnp.where(mask, count, 0.0), axis=0, keepdims=True).astype(jnp.int32)
        slot = lax.rem(e - mine + E, E) * (SPAN // E) + rank
        unpack[...] = one_hot(iota((SPAN, SPAN), 0) == slot)

    at(0.2, prepare_unpack)

    def hot_exact():
        hot_out[...] = joined(nn(thirds(master[...].reshape(2 * W, SPAN)), hot_pick[...]))

    at(0.3, hot_exact)

    def cold_split():
        ins[4].wait()
        cold_three[...] = thirds(cold[...].reshape(2 * W, SPAN))

    at(0.6, cold_split)

    def cold_count():
        for k in range(1, E):
            cs.arrived(shifts.at[es[E - k]], ("s", k))
        rows = iota((E, SPAN), 0)
        mask = shifts[...].reshape(E, SPAN) == lax.rem(rows - e + E, E)
        count = nn(one_hot(mask), before()).astype(jnp.int32)
        count_buf[...] = jnp.where(mask, count, -1)

    at(COLD_TIME, cold_count)

    def cold_pack(b):
        pick = one_hot(iota((SPAN // E, SPAN), 0) == count_buf[b : b + 1])
        cold_sent[b] = joined(nt(cold_three[...], pick))

    for b in range(E):
        at(COLD_TIME + 0.4 + 0.5 * b, functools.partial(cold_pack, b))

    def cold_out():
        for k in range(1, E):
            cs.send(cold_sent.at[es[k]], cold_got.at[e], ("c", k), at_e(k))
        cold_got[e] = cold_sent[e]

    at(COLD_TIME + 0.4 + 0.5 * E, cold_out)

    def turn_tokens(c):
        cols = pl.ds(c * YW, YW)
        tok_t[cols, :] = tok[:, cols].T

    at(0.4, lambda: ins[3].wait())
    for c in range(Z * X):
        at(TURN_TIME + TURN_STEP * c, functools.partial(turn_tokens, c))

    def forward(p):
        def body(c, _):
            cols = pl.ds(pl.multiple_of((zp(p) * X + c) * YW, 128), YW)
            acc[...] += nn(tok[:, cols], wt[zp(p), c].reshape(YW, 2 * H))
            return 0

        lax.fori_loop(0, X, body, 0)

    def clear():
        acc[...] = jnp.zeros_like(acc)

    at(0.5, clear)
    at(t_own + 0.1, lambda: forward(0))
    at(t_far + 0.1, lambda: forward(1))
    run()

    scale = D ** (-0.5)
    TOK = tok.shape[0]
    STEP = 128
    ins[5].wait()
    ins[6].wait()
    count = routed[0]

    def cotangent(i, _):
        rows = pl.ds(pl.multiple_of(i * STEP, STEP), STEP)
        gate = acc[rows, 0:H] * scale
        up = acc[rows, H : 2 * H] * scale
        c = hidden[rows, :].astype(F32)
        live = (iota((STEP, H), 0) + i * STEP) < count
        c = jnp.where(live, c, 0.0)
        sig = jax.nn.sigmoid(gate)
        dmat[rows, H : 2 * H] = (c * gate * sig).astype(BF16)
        dmat[rows, 0:H] = (c * up * sig * (1.0 + gate * (1.0 - sig))).astype(BF16)
        return 0

    lax.fori_loop(0, TOK // STEP, cotangent, 0)

    rs = Family(rs_send_sem, rs_recv_sem)

    def backward(p, kx):
        rows = pl.ds(pl.multiple_of((zp(p) * X + xi(kx)) * YW, 128), YW)
        part[p, xi(kx)] = nn(tok_t[rows, :], dmat[...]).reshape(Y, W, 2 * H)

    def reduce_a(p, t):
        def term(k):
            return part[p, :, yi(k), 0:SPLIT, :]

        def go(i, value, k):
            a_send[p, i] = value.astype(BF16)
            rs.send(a_send.at[p, i], a_recv.at[p, i], ("ay", p, i), at_y(k))

        def come(i):
            rs.arrived(a_recv.at[p, i], ("ay", p, i))
            return a_recv[p, i].astype(F32)

        def begin():
            go(4, term(4), 2)
            go(3, term(3), 1)
            go(6, term(-3), -1)
            go(0, term(1), 1)
            go(5, term(-1), -1)

        def middle():
            go(1, term(2) + come(3) + come(4), 2)
            go(2, term(-2) + come(6), -2)

        def end():
            a_sum[p] = term(0) + come(0) + come(5) + come(1) + come(2)
            for k in range(X):
                if p:
                    rs.send(a_sum.at[p, xi(k)], az_recv.at[k], ("ax", p, k), at_x(k, 1))
                elif k:
                    rs.send(a_sum.at[p, xi(k)], ax_recv.at[k - 1], ("ax", p, k), at_x(k))

        at(t, begin)
        at(t + STEP_TWO + 0.8, middle)
        at(t + 2 * STEP_TWO + 1.5, end)

    HALF = Y // 2

    def reduce_b(p, t):
        def half(h, t):
            cut = pl.ds(h * HALF, HALF)

            def term(k):
                return part[p, xi(k), cut, SPLIT:W, :]

            def go(i, value, k):
                b_send[p, i, cut] = value.astype(BF16)
                rs.send(b_send.at[p, i, cut], b_recv.at[p, i, cut], ("bx", p, i, h), at_x(k))

            def come(i):
                rs.arrived(b_recv.at[p, i, cut], ("bx", p, i, h))
                return b_recv[p, i, cut].astype(F32)

            def begin():
                go(0, term(2), 1)
                go(2, term(-1), -1)

            def middle():
                go(1, term(1) + come(0), 1)

            def end():
                b_sum[p, cut] = term(0) + come(1) + come(2)

            at(t, begin)
            at(t + STEP_ONE + 1.4, middle)
            at(t + 2 * STEP_ONE + 3.0, end)

        half(0, t)
        half(1, t + 0.3)

        def spread():
            if p:
                bz_send[...] = b_sum[p].astype(BF16)
            for k in reversed(far_last):
                if p:
                    rs.send(bz_send.at[yi(k)], bz_recv.at[k], ("by", p, k), at_y(k, 1))
                elif k:
                    rs.send(b_sum.at[p, yi(k)], by_recv.at[k - 1], ("by", p, k), at_y(k))

        at(t + 2 * STEP_ONE + 3.31, spread)

    for i, k in enumerate((2, -1, 1, 0)):
        at(-2.0 + 0.1 * i, functools.partial(backward, 1, k))
        at(0.5 + 0.1 * i, functools.partial(backward, 0, k))
    reduce_b(1, -1.85)
    reduce_a(1, -1.4)
    reduce_b(0, 0.65)
    reduce_a(0, 1.1)

    out_copy = pltpu.make_async_copy(received, received_out, out_sem)

    def cold_in():
        for k in range(1, E):
            cs.arrived(cold_got.at[es[E - k]], ("c", k))
        got = jnp.concatenate([cold_got[c] for c in range(E)], axis=1)
        received[...] = joined(nn(thirds(got), unpack[...]))
        out_copy.start()

    at(COLD_BACK, cold_in)
    run()

    value = a_sum[0, x]
    for k in range(1, X):
        rs.arrived(ax_recv.at[k - 1], ("ax", 0, k))
        value = value + ax_recv[k - 1]
    for k in range(X):
        rs.arrived(az_recv.at[k], ("ax", 1, k))
        value = value + az_recv[k]
    grads_out[0:SPLIT] = value * scale
    value = b_sum[0, y]
    for k in range(1, Y):
        rs.arrived(by_recv.at[k - 1], ("by", 0, k))
        value = value + by_recv[k - 1]
    for k in range(Y):
        rs.arrived(bz_recv.at[k], ("by", 1, k))
        value = value + bz_recv[k].astype(F32)
    grads_out[SPLIT:W] = value * scale
    out_copy.wait()
    for copy in pending:
        copy.wait_send()


def update(grads, m1, m2, hot, master_hot, received, out, m1_out, m2_out):
    _, W, H = m1.shape
    SPAN = received.shape[1]
    pick = one_hot(iota((SPAN, H), 0) == hot[...])
    for i in range(2):
        g = grads[:, i * H : (i + 1) * H]
        first = beta_one * m1[i] + (1.0 - beta_one) * g
        second = beta_two * m2[i] + (1.0 - beta_two) * g * g
        adam = master_hot[i * W : (i + 1) * W] - step_rate * first / (jnp.sqrt(second) + adam_eps)
        m1_out[i] = first
        m2_out[i] = second
        spread = joined(nt(thirds(adam), pick))
        is_hot = nt(jnp.ones((8, H), BF16), pick)[0:1] > 0.5
        out[i] = jnp.where(is_hot, spread, received[i * W : (i + 1) * W])


def per_device(
    tokens, hidden_grads, routed, master, moment_one, moment_two, hot_units, cold_blocks, cold_shift
):
    Z, X, Y = (lax.axis_size(a) for a in DP)
    E = lax.axis_size("expert")
    W = master.shape[2]
    H = hot_units.shape[0]
    SPAN = master.shape[1]
    TOK = tokens.shape[0]
    dims = (Z, X, Y, E, W, H, SPAN)
    vmem = pl.BlockSpec(memory_space=pltpu.VMEM)
    dma = pltpu.SemaphoreType.DMA
    V = pltpu.VMEM
    HI = W - SPLIT
    ag_copies = 2 * ((X + Y) + (Y - 1) + Y * (X - 1))
    rs_copies = 2 * ((Y - 1) + 2 * (X - 1) + X + Y)
    scratch = [
        V((TOK, D), BF16),
        V((TOK, H), BF16),
        pltpu.SMEM((1,), jnp.int32),
        V((2, W, SPAN), F32),
        V((1, H), jnp.int32),
        V((2, W, SPAN), F32),
        V((1, SPAN), jnp.int32),
        V((D, TOK), BF16),
        V((Z, X, Y, W, 2 * H), BF16),
        V((TOK, 2 * H), F32),
        V((TOK, 2 * H), BF16),
        V((2, X, Y, W, 2 * H), F32),
        V((SPAN, H), BF16),
        V((SPAN, SPAN), BF16),
        V((6 * W, SPAN), BF16),
        V((E, 1, SPAN), jnp.int32),
        V((E, SPAN), jnp.int32),
        V((E, 2 * W, SPAN // E), F32),
        V((E, 2 * W, SPAN // E), F32),
        V((2 * W, SPAN), F32),
        V((2, X - 1, Y, HI, 2 * H), BF16),
        V((2, X - 1, Y, HI, 2 * H), BF16),
        V((2, Y - 1, X, SPLIT, 2 * H), BF16),
        V((2, Y - 1, X, SPLIT, 2 * H), BF16),
        V((2, X, SPLIT, 2 * H), F32),
        V((2, Y, HI, 2 * H), F32),
        V((Y, HI, 2 * H), BF16),
        V((Y, HI, 2 * H), BF16),
        V((Y - 1, HI, 2 * H), F32),
        V((X - 1, SPLIT, 2 * H), F32),
        V((X, SPLIT, 2 * H), F32),
        dma((7,)),
        dma,
        dma((ag_copies,)),
        dma((ag_copies,)),
        dma((rs_copies,)),
        dma((rs_copies,)),
        dma((2 * E,)),
        dma((2 * E,)),
    ]

    def turned(v):
        return v.transpose(0, 2, 1)

    hot_row = hot_units.reshape(1, H)
    grads, received, master_hot = pl.pallas_call(
        functools.partial(kernel, dims),
        out_shape=(
            jax.ShapeDtypeStruct((W, 2 * H), F32),
            jax.ShapeDtypeStruct((2 * W, SPAN), F32),
            jax.ShapeDtypeStruct((2 * W, H), F32),
        ),
        in_specs=[pl.BlockSpec(memory_space=pltpu.HBM)] * 7,
        out_specs=(vmem, pl.BlockSpec(memory_space=pltpu.HBM), vmem),
        scratch_shapes=scratch,
        compiler_params=pltpu.CompilerParams(
            collective_id=0, has_side_effects=True, vmem_limit_bytes=60 * 1024 * 1024
        ),
        name="expert_step",
    )(
        tokens,
        hidden_grads,
        routed,
        turned(master),
        hot_row,
        turned(cold_blocks),
        cold_shift.reshape(1, SPAN),
    )
    outs = pl.pallas_call(
        update,
        out_shape=(
            jax.ShapeDtypeStruct((2, W, SPAN), F32),
            jax.ShapeDtypeStruct((2, W, H), F32),
            jax.ShapeDtypeStruct((2, W, H), F32),
        ),
        in_specs=[vmem] * 6,
        out_specs=(vmem, vmem, vmem),
        name="update",
    )(grads, turned(moment_one), turned(moment_two), hot_row, master_hot, received)
    return tuple(turned(v) for v in outs)


def solution(mesh):
    finer = Mesh(
        mesh.devices.reshape(2, 4, 8, mesh.shape["expert"]), ("dp_0", "dp_1", "dp_2", "expert")
    )
    placed = (
        P(DP, None),
        P(DP, "expert"),
        P(DP),
        P(None, "expert", DP),
        P(None, "expert", DP),
        P(None, "expert", DP),
        P("expert"),
        P(None, "expert", DP),
        P("expert"),
    )
    return jax.shard_map(
        per_device,
        mesh=finer,
        in_specs=placed,
        out_specs=(P(None, "expert", DP), P(None, "expert", DP), P(None, "expert", DP)),
        check_vma=False,
    )
```

```python
import functools

import jax
import jax.numpy as jnp
from jax import lax
from jax.experimental import pallas as pl
from jax.experimental.pallas import tpu as pltpu
from jax.sharding import Mesh
from jax.sharding import PartitionSpec as P

D = 3072
DP = ("dp_0", "dp_1", "dp_2")
MESH = pl.DeviceIdType.MESH

beta_one = 0.9
beta_two = 0.95
step_rate = 0.1
adam_eps = 1e-08

SPLIT = 16

STEP_ONE, STEP_TWO = 3.2, 4.2
COLD_TIME = 6.0
TURN_TIME, TURN_STEP = 0.7, 0.35
COLD_BACK = 9.5

F32 = jnp.float32
BF16 = jnp.bfloat16


def nn(a, b):
    return lax.dot_general(a, b, (((1,), (0,)), ((), ())), preferred_element_type=F32)


def nt(a, b):
    return lax.dot_general(a, b, (((1,), (1,)), ((), ())), preferred_element_type=F32)


def thirds(v):
    high = v.astype(BF16)
    rest = v - high.astype(F32)
    mid = rest.astype(BF16)
    low = (rest - mid.astype(F32)).astype(BF16)
    return jnp.concatenate([high, mid, low], axis=0)


def joined(v):
    rows = v.shape[0] // 3
    return v[:rows] + (v[rows : 2 * rows] + v[2 * rows :])


def one_hot(cond):
    return jnp.where(cond, 1.0, 0.0).astype(BF16)


def iota(shape, dim):
    return lax.broadcasted_iota(jnp.int32, shape, dim)


def kernel(
    dims,
    tok_hbm,
    hidden_hbm,
    routed_hbm,
    master_hbm,
    hot_hbm,
    cold_hbm,
    shift_hbm,
    grads_out,
    received_out,
    hot_out,
    tok,
    hidden,
    routed,
    master,
    hot,
    cold,
    shift,
    tok_t,
    wt,
    acc,
    dmat,
    part,
    hot_pick,
    unpack,
    cold_three,
    shifts,
    count_buf,
    cold_sent,
    cold_got,
    received,
    b_send,
    b_recv,
    a_send,
    a_recv,
    a_sum,
    b_sum,
    bz_send,
    bz_recv,
    by_recv,
    ax_recv,
    az_recv,
    in_sem,
    out_sem,
    ag_send_sem,
    ag_recv_sem,
    rs_send_sem,
    rs_recv_sem,
    cold_send_sem,
    cold_recv_sem,
):
    Z, X, Y, E, W, H, SPAN = dims
    YW = Y * W
    z, x, y = (lax.axis_index(a) for a in DP)
    e = lax.axis_index("expert")
    s = 1 - 2 * lax.rem(e, 2)
    xs = [lax.rem(x + k * s + 2 * X, X) for k in range(X)]
    ys = [lax.rem(y + k * s + 2 * Y, Y) for k in range(Y)]
    es = [lax.rem(e + k, E) for k in range(E)]

    def xi(k):
        return xs[k % X]

    def yi(k):
        return ys[k % Y]

    def at_x(k, p=0):
        return (z if p == 0 else 1 - z, xi(k), y, e)

    def at_y(k, p=0):
        return (z if p == 0 else 1 - z, x, yi(k), e)

    def at_e(k):
        return (z, x, y, es[k])

    far_last = sorted(range(Y), key=lambda k: (min(k, Y - k), k))
    peers = [at_x(0, 1)] + [at_y(k) for k in reversed(far_last[1:])]
    peers += [at_x(k) for k in range(1, X)] + [at_e(k) for k in range(1, E)]

    barrier = pltpu.get_barrier_semaphore()
    for peer in peers:
        pl.semaphore_signal(barrier, inc=1, device_id=peer, device_id_type=MESH)
    ins = []
    for i, (src, dst) in enumerate(
        (
            (hot_hbm, hot),
            (master_hbm, master),
            (shift_hbm, shift),
            (tok_hbm, tok),
            (cold_hbm, cold),
            (hidden_hbm, hidden),
            (routed_hbm, routed),
        )
    ):
        ins.append(pltpu.make_async_copy(src, dst, in_sem.at[i]))
    for copy in ins[:3]:
        copy.start()

    for copy in ins[:3]:
        copy.wait()
    for copy in ins[3:]:
        copy.start()
    hot_pick[...] = one_hot(iota((SPAN, H), 0) == hot[...])
    whole = master[...].reshape(2 * W, SPAN)
    picked = nn(whole.astype(BF16), hot_pick[...]).astype(BF16)
    wt[z, x, y, :, 0:H] = picked[:W]
    wt[z, x, y, :, H : 2 * H] = picked[W:]
    shifts[e] = shift[...]

    pl.semaphore_wait(barrier, len(peers))

    pending = []

    class Family:
        def __init__(self, send_sem, recv_sem):
            self.sems = (send_sem, recv_sem)
            self.names = {}

        def copy(self, src, dst, name, peer):
            k = self.names.setdefault(name, len(self.names))
            assert k < self.sems[0].shape[0]
            return pltpu.make_async_remote_copy(
                src_ref=src,
                dst_ref=dst,
                send_sem=self.sems[0].at[k],
                recv_sem=self.sems[1].at[k],
                device_id=peer,
                device_id_type=MESH,
            )

        def send(self, src, dst, name, peer):
            copy = self.copy(src, dst, name, peer)
            copy.start()
            pending.append(copy)

        def arrived(self, dst, name):
            self.copy(dst, dst, name, at_x(0, 1)).wait_recv()

    events = []

    def at(t, fn):
        events.append((t, len(events), fn))

    def run():
        for _, _, fn in sorted(events, key=lambda ev: ev[:2]):
            fn()
        events.clear()

    low, high = pl.ds(0, SPLIT), pl.ds(SPLIT, W - SPLIT)

    ag = Family(ag_send_sem, ag_recv_sem)

    def zp(p):
        return z if p == 0 else 1 - z

    def first_sends(p):
        mine = wt.at[zp(p), x, y]
        if p:
            ag.arrived(mine, ("z",))
        else:
            ag.send(mine, mine, ("z",), at_x(0, 1))
        mine_a, mine_b = wt.at[zp(p), x, y, low], wt.at[zp(p), x, y, high]
        for k in range(1, X):
            ag.send(mine_a, mine_a, ("ax", p, k), at_x(k))
        for k in far_last[1:]:
            ag.send(mine_b, mine_b, ("by", p, k), at_y(k))

    Z_TIME = 5.8
    at(0.0, lambda: first_sends(0))
    at(Z_TIME, lambda: first_sends(1))

    def gather_a(p, t):
        def row(k):
            return wt.at[zp(p), :, yi(k), low]

        def begin():
            for k in range(1, X):
                ag.arrived(wt.at[zp(p), xi(-k), y, low], ("ax", p, k))
            for k in (2, 1, -2, -1):
                ag.send(row(0), row(0), ("ay", p, k), at_y(k))

        def near():
            for k in (1, -1):
                ag.arrived(row(-k), ("ay", p, k))

        def relay():
            ag.arrived(row(-2), ("ay", p, 2))
            ag.send(row(-2), row(-2), ("ay", p, 4), at_y(2))
            ag.send(row(-2), row(-2), ("ay", p, 3), at_y(1))
            ag.arrived(row(2), ("ay", p, -2))
            ag.send(row(2), row(2), ("ay", p, -3), at_y(-1))

        def end():
            for k in (3, -3, 4):
                ag.arrived(row(-k), ("ay", p, k))

        at(t, begin)
        at(t + STEP_TWO + 0.4, relay)
        at(t + STEP_TWO + 0.6, near)
        at(t + 2 * STEP_TWO + 1.5, end)
        return t + 2 * STEP_TWO + 1.5

    def gather_b(p, t, ky):
        def piece(kx):
            return wt.at[zp(p), xi(kx), yi(-ky), high]

        def begin():
            if ky:
                ag.arrived(piece(0), ("by", p, ky))
            ag.send(piece(0), piece(0), ("bx", p, ky, 1), at_x(1))
            ag.send(piece(0), piece(0), ("bx", p, ky, -1), at_x(-1))

        def relay():
            ag.arrived(piece(-1), ("bx", p, ky, 1))
            ag.send(piece(-1), piece(-1), ("bx", p, ky, 2), at_x(1))

        def end():
            ag.arrived(piece(1), ("bx", p, ky, -1))
            ag.arrived(piece(-2), ("bx", p, ky, 2))

        at(t, begin)
        at(t + STEP_ONE + 0.3, relay)
        at(t + 2 * STEP_ONE + 0.8, end)
        return t + 2 * STEP_ONE + 0.8

    ends = [[gather_a(0, 4.3)], [gather_a(1, Z_TIME + 4.3)]]
    for i, k in enumerate(far_last):
        d = min(k, Y - k)
        for p in range(2):
            t = 0.01 if k == 0 else 2.4 + 0.8 * d + 0.3 * i
            ends[p].append(gather_b(p, t + p * Z_TIME, k))
    t_own, t_far = max(ends[0]), max(ends[1])

    cs = Family(cold_send_sem, cold_recv_sem)

    def shift_out():
        for k in range(1, E):
            cs.send(shift, shifts.at[e], ("s", k), at_e(k))

    at(0.02, shift_out)

    def before():
        return one_hot(iota((SPAN, SPAN), 0) < iota((SPAN, SPAN), 1))

    def prepare_unpack():
        mine = shift[...]
        rows = iota((E, SPAN), 0)
        mask = mine == rows
        count = nn(one_hot(mask), before())
        rank = jnp.sum(jnp.where(mask, count, 0.0), axis=0, keepdims=True).astype(jnp.int32)
        slot = lax.rem(e - mine + E, E) * (SPAN // E) + rank
        unpack[...] = one_hot(iota((SPAN, SPAN), 0) == slot)

    at(0.2, prepare_unpack)

    def hot_exact():
        hot_out[...] = joined(nn(thirds(master[...].reshape(2 * W, SPAN)), hot_pick[...]))

    at(0.3, hot_exact)

    def cold_split():
        ins[4].wait()
        cold_three[...] = thirds(cold[...].reshape(2 * W, SPAN))

    at(0.6, cold_split)

    def cold_count():
        for k in range(1, E):
            cs.arrived(shifts.at[es[E - k]], ("s", k))
        rows = iota((E, SPAN), 0)
        mask = shifts[...].reshape(E, SPAN) == lax.rem(rows - e + E, E)
        count = nn(one_hot(mask), before()).astype(jnp.int32)
        count_buf[...] = jnp.where(mask, count, -1)

    at(COLD_TIME, cold_count)

    def cold_pack(b):
        pick = one_hot(iota((SPAN // E, SPAN), 0) == count_buf[b : b + 1])
        cold_sent[b] = joined(nt(cold_three[...], pick))

    for b in range(E):
        at(COLD_TIME + 0.4 + 0.25 * b, functools.partial(cold_pack, b))

    def cold_out():
        for k in range(1, E):
            cs.send(cold_sent.at[es[k]], cold_got.at[e], ("c", k), at_e(k))
        cold_got[e] = cold_sent[e]

    at(COLD_TIME + 0.4 + 0.25 * E, cold_out)

    def turn_tokens(c):
        cols = pl.ds(c * YW, YW)
        tok_t[cols, :] = tok[:, cols].T

    at(0.4, lambda: ins[3].wait())
    for c in range(Z * X):
        at(TURN_TIME + TURN_STEP * c, functools.partial(turn_tokens, c))

    def forward(p):
        def body(c, _):
            cols = pl.ds(pl.multiple_of((zp(p) * X + c) * YW, 128), YW)
            acc[...] += nn(tok[:, cols], wt[zp(p), c].reshape(YW, 2 * H))
            return 0

        lax.fori_loop(0, X, body, 0)

    def clear():
        acc[...] = jnp.zeros_like(acc)

    at(0.5, clear)
    at(t_own + 0.1, lambda: forward(0))
    at(t_far + 0.1, lambda: forward(1))
    run()

    scale = D ** (-0.5)
    TOK = tok.shape[0]
    STEP = 128
    ins[5].wait()
    ins[6].wait()
    count = routed[0]

    def cotangent(i, _):
        rows = pl.ds(pl.multiple_of(i * STEP, STEP), STEP)
        gate = acc[rows, 0:H] * scale
        up = acc[rows, H : 2 * H] * scale
        c = hidden[rows, :].astype(F32)
        live = (iota((STEP, H), 0) + i * STEP) < count
        c = jnp.where(live, c, 0.0)
        sig = jax.nn.sigmoid(gate)
        dmat[rows, H : 2 * H] = (c * gate * sig).astype(BF16)
        dmat[rows, 0:H] = (c * up * sig * (1.0 + gate * (1.0 - sig))).astype(BF16)
        return 0

    lax.fori_loop(0, TOK // STEP, cotangent, 0)

    rs = Family(rs_send_sem, rs_recv_sem)

    def backward(p, kx):
        rows = pl.ds(pl.multiple_of((zp(p) * X + xi(kx)) * YW, 128), YW)
        part[p, xi(kx)] = nn(tok_t[rows, :], dmat[...]).reshape(Y, W, 2 * H)

    def reduce_a(p, t):
        def term(k):
            return part[p, :, yi(k), 0:SPLIT, :]

        def go(i, value, k):
            a_send[p, i] = value.astype(BF16)
            rs.send(a_send.at[p, i], a_recv.at[p, i], ("ay", p, i), at_y(k))

        def come(i):
            rs.arrived(a_recv.at[p, i], ("ay", p, i))
            return a_recv[p, i].astype(F32)

        def begin():
            go(4, term(4), 2)
            go(3, term(3), 1)
            go(6, term(-3), -1)
            go(0, term(1), 1)
            go(5, term(-1), -1)

        def middle():
            go(1, term(2) + come(3) + come(4), 2)
            go(2, term(-2) + come(6), -2)

        def end():
            a_sum[p] = term(0) + come(0) + come(5) + come(1) + come(2)
            for k in range(X):
                if p:
                    rs.send(a_sum.at[p, xi(k)], az_recv.at[k], ("ax", p, k), at_x(k, 1))
                elif k:
                    rs.send(a_sum.at[p, xi(k)], ax_recv.at[k - 1], ("ax", p, k), at_x(k))

        at(t, begin)
        at(t + STEP_TWO + 0.8, middle)
        at(t + 2 * STEP_TWO + 1.5, end)

    HALF = Y // 2

    def reduce_b(p, t):
        def half(h, t):
            cut = pl.ds(h * HALF, HALF)

            def term(k):
                return part[p, xi(k), cut, SPLIT:W, :]

            def go(i, value, k):
                b_send[p, i, cut] = value.astype(BF16)
                rs.send(b_send.at[p, i, cut], b_recv.at[p, i, cut], ("bx", p, i, h), at_x(k))

            def come(i):
                rs.arrived(b_recv.at[p, i, cut], ("bx", p, i, h))
                return b_recv[p, i, cut].astype(F32)

            def begin():
                go(0, term(2), 1)
                go(2, term(-1), -1)

            def middle():
                go(1, term(1) + come(0), 1)

            def end():
                b_sum[p, cut] = term(0) + come(1) + come(2)

            at(t, begin)
            at(t + STEP_ONE + 1.4, middle)
            at(t + 2 * STEP_ONE + 3.0, end)

        half(0, t)
        half(1, t + 0.3)

        def spread():
            if p:
                bz_send[...] = b_sum[p].astype(BF16)
            for k in reversed(far_last):
                if p:
                    rs.send(bz_send.at[yi(k)], bz_recv.at[k], ("by", p, k), at_y(k, 1))
                elif k:
                    rs.send(b_sum.at[p, yi(k)], by_recv.at[k - 1], ("by", p, k), at_y(k))

        at(t + 2 * STEP_ONE + 3.31, spread)

    for i, k in enumerate((2, -1, 1, 0)):
        at(-2.0 + 0.1 * i, functools.partial(backward, 1, k))
        at(0.5 + 0.1 * i, functools.partial(backward, 0, k))
    reduce_b(1, -1.85)
    reduce_a(1, -1.4)
    reduce_b(0, 0.65)
    reduce_a(0, 1.1)

    out_copy = pltpu.make_async_copy(received, received_out, out_sem)

    def cold_in():
        for k in range(1, E):
            cs.arrived(cold_got.at[es[E - k]], ("c", k))
        got = jnp.concatenate([cold_got[c] for c in range(E)], axis=1)
        received[...] = joined(nn(thirds(got), unpack[...]))
        out_copy.start()

    at(COLD_BACK, cold_in)
    run()

    value = a_sum[0, x]
    for k in range(1, X):
        rs.arrived(ax_recv.at[k - 1], ("ax", 0, k))
        value = value + ax_recv[k - 1]
    for k in range(X):
        rs.arrived(az_recv.at[k], ("ax", 1, k))
        value = value + az_recv[k]
    grads_out[0:SPLIT] = value * scale
    value = b_sum[0, y]
    for k in range(1, Y):
        rs.arrived(by_recv.at[k - 1], ("by", 0, k))
        value = value + by_recv[k - 1]
    for k in range(Y):
        rs.arrived(bz_recv.at[k], ("by", 1, k))
        value = value + bz_recv[k].astype(F32)
    grads_out[SPLIT:W] = value * scale
    out_copy.wait()
    for copy in pending:
        copy.wait_send()


def update(grads, m1, m2, hot, master_hot, received, out, m1_out, m2_out):
    _, W, H = m1.shape
    SPAN = received.shape[1]
    pick = one_hot(iota((SPAN, H), 0) == hot[...])
    for i in range(2):
        g = grads[:, i * H : (i + 1) * H]
        first = beta_one * m1[i] + (1.0 - beta_one) * g
        second = beta_two * m2[i] + (1.0 - beta_two) * g * g
        adam = master_hot[i * W : (i + 1) * W] - step_rate * first / (jnp.sqrt(second) + adam_eps)
        m1_out[i] = first
        m2_out[i] = second
        spread = joined(nt(thirds(adam), pick))
        is_hot = nt(jnp.ones((8, H), BF16), pick)[0:1] > 0.5
        out[i] = jnp.where(is_hot, spread, received[i * W : (i + 1) * W])


def per_device(
    tokens, hidden_grads, routed, master, moment_one, moment_two, hot_units, cold_blocks, cold_shift
):
    Z, X, Y = (lax.axis_size(a) for a in DP)
    E = lax.axis_size("expert")
    W = master.shape[2]
    H = hot_units.shape[0]
    SPAN = master.shape[1]
    TOK = tokens.shape[0]
    dims = (Z, X, Y, E, W, H, SPAN)
    vmem = pl.BlockSpec(memory_space=pltpu.VMEM)
    dma = pltpu.SemaphoreType.DMA
    V = pltpu.VMEM
    HI = W - SPLIT
    ag_copies = 2 * ((X + Y) + (Y - 1) + Y * (X - 1))
    rs_copies = 2 * ((Y - 1) + 2 * (X - 1) + X + Y)
    scratch = [
        V((TOK, D), BF16),
        V((TOK, H), BF16),
        pltpu.SMEM((1,), jnp.int32),
        V((2, W, SPAN), F32),
        V((1, H), jnp.int32),
        V((2, W, SPAN), F32),
        V((1, SPAN), jnp.int32),
        V((D, TOK), BF16),
        V((Z, X, Y, W, 2 * H), BF16),
        V((TOK, 2 * H), F32),
        V((TOK, 2 * H), BF16),
        V((2, X, Y, W, 2 * H), F32),
        V((SPAN, H), BF16),
        V((SPAN, SPAN), BF16),
        V((6 * W, SPAN), BF16),
        V((E, 1, SPAN), jnp.int32),
        V((E, SPAN), jnp.int32),
        V((E, 2 * W, SPAN // E), F32),
        V((E, 2 * W, SPAN // E), F32),
        V((2 * W, SPAN), F32),
        V((2, X - 1, Y, HI, 2 * H), BF16),
        V((2, X - 1, Y, HI, 2 * H), BF16),
        V((2, Y - 1, X, SPLIT, 2 * H), BF16),
        V((2, Y - 1, X, SPLIT, 2 * H), BF16),
        V((2, X, SPLIT, 2 * H), F32),
        V((2, Y, HI, 2 * H), F32),
        V((Y, HI, 2 * H), BF16),
        V((Y, HI, 2 * H), BF16),
        V((Y - 1, HI, 2 * H), F32),
        V((X - 1, SPLIT, 2 * H), F32),
        V((X, SPLIT, 2 * H), F32),
        dma((7,)),
        dma,
        dma((ag_copies,)),
        dma((ag_copies,)),
        dma((rs_copies,)),
        dma((rs_copies,)),
        dma((2 * E,)),
        dma((2 * E,)),
    ]

    def turned(v):
        return v.transpose(0, 2, 1)

    hot_row = hot_units.reshape(1, H)
    grads, received, master_hot = pl.pallas_call(
        functools.partial(kernel, dims),
        out_shape=(
            jax.ShapeDtypeStruct((W, 2 * H), F32),
            jax.ShapeDtypeStruct((2 * W, SPAN), F32),
            jax.ShapeDtypeStruct((2 * W, H), F32),
        ),
        in_specs=[pl.BlockSpec(memory_space=pltpu.HBM)] * 7,
        out_specs=(vmem, pl.BlockSpec(memory_space=pltpu.HBM), vmem),
        scratch_shapes=scratch,
        compiler_params=pltpu.CompilerParams(
            collective_id=0, has_side_effects=True, vmem_limit_bytes=60 * 1024 * 1024
        ),
        name="expert_step",
    )(
        tokens,
        hidden_grads,
        routed,
        turned(master),
        hot_row,
        turned(cold_blocks),
        cold_shift.reshape(1, SPAN),
    )
    outs = pl.pallas_call(
        update,
        out_shape=(
            jax.ShapeDtypeStruct((2, W, SPAN), F32),
            jax.ShapeDtypeStruct((2, W, H), F32),
            jax.ShapeDtypeStruct((2, W, H), F32),
        ),
        in_specs=[vmem] * 6,
        out_specs=(vmem, vmem, vmem),
        name="update",
    )(grads, turned(moment_one), turned(moment_two), hot_row, master_hot, received)
    return tuple(turned(v) for v in outs)


def solution(mesh):
    finer = Mesh(
        mesh.devices.reshape(2, 4, 8, mesh.shape["expert"]), ("dp_0", "dp_1", "dp_2", "expert")
    )
    placed = (
        P(DP, None),
        P(DP, "expert"),
        P(DP),
        P(None, "expert", DP),
        P(None, "expert", DP),
        P(None, "expert", DP),
        P("expert"),
        P(None, "expert", DP),
        P("expert"),
    )
    return jax.shard_map(
        per_device,
        mesh=finer,
        in_specs=placed,
        out_specs=(P(None, "expert", DP), P(None, "expert", DP), P(None, "expert", DP)),
        check_vma=False,
    )
```
